16 devices in a mesh: dp: 2 (over y, z), tp: 8 (over x, core).
Axes of the slice: x: 4, y: 2, z: 1, core: 2. Of those that a mesh axis runs over, the one named last changes fastest.
The devices are a block of a 4x4x4 slice.
Arguments:
- x: bfloat16 [128, 8192], P('dp'), parts along dimension 0
- k_cache: bfloat16 [128, 4096, 8, 128], P('dp', None, 'tp'), parts along dimension 0
- v_cache: bfloat16 [128, 4096, 8, 128], P('dp', None, 'tp'), parts along dimension 0
- gain_a: bfloat16 [8192], replicated
- wq: bfloat16 [8192, 8192], P(None, 'tp')
- wo: bfloat16 [8192, 8192], P('tp')
- gain_m: bfloat16 [8192], replicated
- w_gate: bfloat16 [8192, 49152], P(None, 'tp')
- w_up: bfloat16 [8192, 49152], P(None, 'tp')
- w_down: bfloat16 [49152, 8192], P('tp')
Outputs:
- output: bfloat16 [128, 8192], P('dp'), parts along dimension 0
There are 2 independent parts. The reference program is written for one: setup_inputs(seed, part) draws one part's arguments, and reference() takes and returns one part's arrays. A program takes and returns all parts, laid end to end along the dimension named above; an argument that names none is the same for every part.
All inputs are finite; a program needn't handle non-finite values.
Results may differ from the reference program's by a relative error of at most 0.017.
Values are sent between devices in bfloat16 or wider.
A program may use at most 1.5 GiB of HBM per device.

```python
import jax
import jax.numpy as jnp
from jax import lax

BATCH = 64
CACHE = 4096
D = 8192
HEADS = 64
KV_HEADS = 8
HEAD = 128
FF = 49152
THETA = 10000


def setup_inputs(seed: int = 0, part: int = 0) -> dict:
    kx, kc, kw, kn, kq, ko, km, kg, ku, kd = jax.random.split(jax.random.key(seed), 10)
    kx, kc, kw = (jax.random.fold_in(k, part) for k in (kx, kc, kw))

    def weights(key, rows, columns):
        return jax.random.normal(key, (rows, columns), jnp.float32) * rows**-0.5

    drawn = {
        "x": jax.random.normal(kx, (BATCH, D), jnp.float32),
        "k_cache": 2 * jax.random.normal(kc, (BATCH, CACHE, KV_HEADS, HEAD), jnp.float32),
        "v_cache": 4 * jax.random.normal(kw, (BATCH, CACHE, KV_HEADS, HEAD), jnp.float32),
        "gain_a": 1 + 0.1 * jax.random.normal(kn, (D,), jnp.float32),
        "wq": 2 * weights(kq, D, HEADS * HEAD),
        "wo": weights(ko, HEADS * HEAD, D),
        "gain_m": 1 + 0.1 * jax.random.normal(km, (D,), jnp.float32),
        "w_gate": weights(kg, D, FF),
        "w_up": weights(ku, D, FF),
        "w_down": 2 * weights(kd, FF, D),
    }
    return {k: v.astype(jnp.bfloat16) for k, v in drawn.items()}


def normed(x, gain):
    wide = x.astype(jnp.float32)
    scale = lax.rsqrt(jnp.mean(wide * wide, -1, keepdims=True) + 1e-6)
    return (wide * scale * gain.astype(jnp.float32)).astype(jnp.bfloat16)


def turned(t, place, theta):
    half = t.shape[-1] // 2
    angle = place.astype(jnp.float32)[:, None] * theta ** (-jnp.arange(half, dtype=jnp.float32) / half)
    cos, sin = jnp.cos(angle)[:, None], jnp.sin(angle)[:, None]
    a, b = t[..., :half].astype(jnp.float32), t[..., half:].astype(jnp.float32)
    return jnp.concatenate([a * cos - b * sin, b * cos + a * sin], -1).astype(jnp.bfloat16)


def matmul(a, w):
    return jnp.dot(a, w, preferred_element_type=jnp.float32).astype(jnp.bfloat16)


def einsum(form, a, b):
    return jnp.einsum(form, a.astype(jnp.float32), b.astype(jnp.float32))


def seen_by(a, wq, k_cache, v_cache, head, theta):
    batch, cache, kv_heads = k_cache.shape[:3]
    place = jnp.full((batch,), cache - 1)
    q = turned(matmul(a, wq).reshape(batch, -1, head), place, theta).reshape(batch, kv_heads, -1, head)
    scores = einsum("bgsd,bugd->bgsu", q, k_cache) * head**-0.5
    weights = jax.nn.softmax(scores, -1).astype(jnp.bfloat16)
    return einsum("bgsu,bugd->bgsd", weights, v_cache).astype(jnp.bfloat16).reshape(batch, -1)


def hidden_of(b, w_gate, w_up):
    gate = jnp.dot(b, w_gate, preferred_element_type=jnp.float32)
    up = jnp.dot(b, w_up, preferred_element_type=jnp.float32)
    return (jax.nn.silu(gate) * up).astype(jnp.bfloat16)


def reference(x, k_cache, v_cache, gain_a, wq, wo, gain_m, w_gate, w_up, w_down):
    seen = seen_by(normed(x, gain_a), wq, k_cache, v_cache, HEAD, THETA)
    h = (x.astype(jnp.float32) + jnp.dot(seen, wo, preferred_element_type=jnp.float32)).astype(jnp.bfloat16)
    hidden = hidden_of(normed(h, gain_m), w_gate, w_up)
    return (h.astype(jnp.float32) + jnp.dot(hidden, w_down, preferred_element_type=jnp.float32)).astype(jnp.bfloat16)
```

```python
import functools

import jax
import jax.numpy as jnp
import numpy as np
from jax import lax
from jax.experimental import pallas as pl
from jax.experimental.pallas import tpu as pltpu
from jax.sharding import PartitionSpec as P

HEAD = 128
THETA = 10000
LANES = 128
WIDTH = 256
SLOTS = 12
CORES = 2
F32, BF16 = jnp.float32, jnp.bfloat16
MESH = pl.DeviceIdType.MESH


def layer(n, dims, x_hbm, k_hbm, v_hbm, ga_ref, gm_ref, rot_ref, wq_hbm, wo_hbm, wg_hbm, wu_hbm, wd_hbm, y_ref,
          ring, xbuf, normed, hbuf, gain, q, seen, seen_bf, hidden, pbuf, sbuf, dbuf, tbuf, rbuf,
          ring_sem, x_sem, s_a, r_a, s_b, r_b, s_c, r_c, s_d, r_d):
    rows, d, cache, qcols, ff = dims
    heads = qcols // HEAD
    half_cache = cache // 2
    group = d // half_cache
    chips = n // CORES
    chunk = CORES * chips * LANES
    chunks = d // chunk
    core_cols = chips * LANES
    wo_cols = d // qcols * WIDTH
    per_item = wo_cols // chunk

    n_q, n_kv, n_wo, n_gu, n_wd = qcols // WIDTH, 2 * rows // group, d // wo_cols, 2 * ff // WIDTH, d // WIDTH
    kv0 = n_q
    wo0 = kv0 + n_kv
    gu0 = wo0 + n_wo
    wd0 = gu0 + n_gu
    end = wd0 + n_wd

    me = lax.axis_index("tp")
    chip, core = me // CORES, me % CORES
    partner = chip * CORES + (1 - core)

    def peer(distance):
        return lax.rem(chip + distance, chips) * CORES + core

    def columns(start, size):
        return pl.ds(pl.multiple_of(start, size), size)

    def slot(i):
        return i % SLOTS if isinstance(i, int) else lax.rem(i, SLOTS)

    def issue(i, phases):
        s = slot(i)
        sem = ring_sem.at[s]

        def cols_of(w, block, height):
            pltpu.make_async_copy(w.at[:, columns(block * WIDTH, WIDTH)], ring.at[s, pl.ds(0, height)], sem).start()

        def caches(src, g):
            for t in range(group):
                for h in range(2):
                    pltpu.make_async_copy(
                        src.at[g * group + t, pl.ds(h * half_cache, half_cache)],
                        ring.at[s, pl.ds(t * half_cache, half_cache), pl.ds(h * HEAD, HEAD)],
                        sem,
                    ).start()

        def wo_blocks(w):
            for m in range(wo_cols // WIDTH):
                pltpu.make_async_copy(
                    wo_hbm.at[:, columns(w * wo_cols + m * WIDTH, WIDTH)], ring.at[s, pl.ds(m * qcols, qcols)], sem
                ).start()

        def when(low, high, body):
            if isinstance(i, int):
                if low <= i < high:
                    body()
            else:
                pl.when((i >= low) & (i < high))(body)

        def either(first, second, j):
            if isinstance(j, int):
                (second if j % 2 else first)(j // 2)
            else:
                pl.when(j % 2 == 0)(lambda: first(j // 2))
                pl.when(j % 2 == 1)(lambda: second(j // 2))

        if "q" in phases:
            when(0, kv0, lambda: cols_of(wq_hbm, i, d))
        if "kv" in phases:
            when(kv0, wo0, lambda: either(lambda g: caches(k_hbm, g), lambda g: caches(v_hbm, g), i - kv0))
        if "wo" in phases:
            when(wo0, gu0, lambda: wo_blocks(i - wo0))
        if "gu" in phases:
            when(gu0, wd0, lambda: either(lambda j: cols_of(wg_hbm, j, d), lambda j: cols_of(wu_hbm, j, d), i - gu0))
        if "wd" in phases:
            when(wd0, end, lambda: cols_of(wd_hbm, i - wd0, ff))

    def arrived(i, height=d):
        s = slot(i)
        src = wd_hbm if height == ff else wg_hbm
        pltpu.make_async_copy(src.at[:, pl.ds(0, WIDTH)], ring.at[s, pl.ds(0, height)], ring_sem.at[s]).wait()
        return s

    def product(a_ref, s, depth, start=0, step=2048):
        total = None
        for k in range(0, depth, step):
            size = min(step, depth - k)
            part = jnp.dot(a_ref[:, k : k + size], ring[s, start + k : start + k + size], preferred_element_type=F32)
            total = part if total is None else total + part
        return total

    barrier = pltpu.get_barrier_semaphore()
    for device in [partner] + [peer(dist) for dist in range(1, chips)]:
        pl.semaphore_signal(barrier, inc=1, device_id={"tp": device}, device_id_type=MESH)
    x_copy = pltpu.make_async_copy(x_hbm, xbuf, x_sem)
    x_copy.start()
    for i in range(SLOTS):
        issue(i, ("q", "kv"))

    def norm(src_ref, gain_ref):
        gain[...] = gain_ref[...].astype(F32)
        block = 2 * LANES

        def square(r, acc):
            v = src_ref[:, columns(r * block, block)].astype(F32)
            v = v * v
            return acc + (v[:, :LANES] + v[:, LANES:])

        acc = lax.fori_loop(0, d // block, square, jnp.zeros((rows, LANES), F32), unroll=4)
        scale = lax.rsqrt(jnp.sum(acc, -1, keepdims=True) * (1.0 / d) + 1e-6)
        scale = jnp.broadcast_to(scale, (rows, LANES))

        def apply(r, _):
            at = columns(r * LANES, LANES)
            normed[:, at] = (src_ref[:, at].astype(F32) * scale * gain[pl.ds(r, 1), :]).astype(BF16)
            return 0

        lax.fori_loop(0, d // LANES, apply, 0, unroll=4)

    x_copy.wait()
    norm(xbuf, ga_ref)

    def queries(i, _):
        s = arrived(i)
        t = product(normed, s, d).astype(BF16).astype(F32)
        cos, sin = rot_ref[0:1, :], rot_ref[1:2, :]
        for j in range(WIDTH // HEAD):
            one = t[:, j * HEAD : (j + 1) * HEAD]
            turned = one * cos + pltpu.roll(one, HEAD // 2, 1) * sin
            q[pl.ds(i * (WIDTH // HEAD) + j, rows, stride=heads), :] = turned.astype(BF16).astype(F32)
        issue(i + SLOTS, ("kv",))
        return 0

    lax.fori_loop(0, n_q, queries, 0)

    def attend(g, _):
        i = kv0 + 2 * g
        sk = arrived(i)
        sv = arrived(i + 1)
        weights = []
        for t in range(group):
            qb = q[pl.ds(pl.multiple_of((g * group + t) * heads, heads), heads), :]
            zero = jnp.zeros_like(qb)
            both = jnp.concatenate([jnp.concatenate([qb, zero], 1), jnp.concatenate([zero, qb], 1)], 0).astype(BF16)
            keys = ring[sk, t * half_cache : (t + 1) * half_cache]
            scores = lax.dot_general(both, keys, (((1,), (1,)), ((), ())), preferred_element_type=F32) * HEAD**-0.5
            top = jnp.max(scores, -1, keepdims=True)
            top = jnp.maximum(top[:heads], top[heads:])
            e = jnp.exp(scores - jnp.concatenate([top, top], 0))
            total = jnp.sum(e, -1, keepdims=True)
            total = 1.0 / (total[:heads] + total[heads:])
            weights.append((e * jnp.concatenate([total, total], 0)).astype(BF16))
        for t in range(group):
            values = ring[sv, t * half_cache : (t + 1) * half_cache]
            out = jnp.dot(weights[t], values, preferred_element_type=F32)
            seen[pl.ds(g * group + t, heads, stride=rows), :] = out[:heads, :HEAD] + out[heads:, HEAD:]
        issue(i + SLOTS, ("kv", "wo", "gu"))
        issue(i + 1 + SLOTS, ("kv", "wo", "gu"))
        return 0

    lax.fori_loop(0, rows // group, attend, 0)
    for h in range(heads):
        seen_bf[:, h * HEAD : (h + 1) * HEAD] = seen[h * rows : (h + 1) * rows, :].astype(BF16)

    def half_to_partner(ph, c):
        return pltpu.make_async_remote_copy(
            src_ref=sbuf.at[c], dst_ref=dbuf.at[c], send_sem=s_a.at[ph, c], recv_sem=r_a.at[ph, c],
            device_id={"tp": partner}, device_id_type=MESH)

    def term_to(ph, c, dist):
        return pltpu.make_async_remote_copy(
            src_ref=tbuf.at[c, lax.rem(chip + dist, chips)], dst_ref=rbuf.at[c, dist - 1],
            send_sem=s_b.at[ph, c, dist - 1], recv_sem=r_b.at[ph, c, dist - 1],
            device_id={"tp": peer(dist)}, device_id_type=MESH)

    def own_columns(c):
        return columns(c * chunk + core * core_cols + chip * LANES, LANES)

    def result_to(dst, ph, c, dist):
        return pltpu.make_async_remote_copy(
            src_ref=dst.at[:, own_columns(c)], dst_ref=dst.at[:, own_columns(c)],
            send_sem=s_c.at[ph, c, dist - 1], recv_sem=r_c.at[ph, c, dist - 1],
            device_id={"tp": peer(dist)}, device_id_type=MESH)

    def results_to_partner(dst, ph, c):
        at = columns(c * chunk + core * core_cols, core_cols)
        return pltpu.make_async_remote_copy(
            src_ref=dst.at[:, at], dst_ref=dst.at[:, at], send_sem=s_d.at[ph, c], recv_sem=r_d.at[ph, c],
            device_id={"tp": partner}, device_id_type=MESH)

    def stage_a(ph, c):
        sbuf[c] = pbuf[c, 1 - core].astype(BF16)
        half_to_partner(ph, c).start()

    def stage_b(ph, c):
        half_to_partner(ph, c).wait_recv()
        both = pbuf[c, core] + dbuf[c].astype(F32)
        pbuf[c, core] = both
        for p in range(chips):
            tbuf[c, p] = both[:, p * LANES : (p + 1) * LANES].astype(BF16)
        for dist in range(1, chips):
            term_to(ph, c, dist).start()

    def stage_c(ph, c, res, dst):
        for dist in range(1, chips):
            term_to(ph, c, dist).wait_recv()
        total = pbuf[c, core, :, columns(chip * LANES, LANES)]
        for dist in range(1, chips):
            total = total + rbuf[c, dist - 1].astype(F32)
        at = own_columns(c)
        dst[:, at] = (res[:, at].astype(F32) + total).astype(BF16)
        for dist in range(1, chips):
            result_to(dst, ph, c, dist).start()

    def stage_d(ph, c, dst):
        for dist in range(1, chips):
            result_to(dst, ph, c, dist).wait_recv()
        results_to_partner(dst, ph, c).start()

    def finish(ph, c, dst):
        results_to_partner(dst, ph, c).wait()
        half_to_partner(ph, c).wait_send()
        for dist in range(1, chips):
            term_to(ph, c, dist).wait_send()
            result_to(dst, ph, c, dist).wait_send()

    def loop(low, high, body):
        lax.fori_loop(low, high, lambda c, _: (body(c), 0)[1], 0)

    pl.semaphore_wait(barrier, chips)

    def project(w, _):
        i = wo0 + w
        s = arrived(i)
        for m in range(wo_cols // WIDTH):
            c = w * per_item + m * WIDTH // chunk
            at = m * WIDTH % chunk
            part = product(seen_bf, s, qcols, m * qcols)
            pbuf[c, at // core_cols, :, at % core_cols : at % core_cols + WIDTH] = part
            if (m + 1) * WIDTH % chunk == 0:
                stage_a(0, c)
        issue(i + SLOTS, ("gu",))

        @pl.when(w >= 1)
        def _():
            for j in range(per_item):
                stage_b(0, (w - 1) * per_item + j)

        @pl.when(w >= 2)
        def _():
            for j in range(per_item):
                stage_c(0, (w - 2) * per_item + j, xbuf, hbuf)

        return 0

    lax.fori_loop(0, n_wo, project, 0)
    loop((n_wo - 1) * per_item, chunks, lambda c: stage_b(0, c))
    loop((n_wo - 2) * per_item, (n_wo - 1) * per_item, lambda c: stage_c(0, c, xbuf, hbuf))
    loop(0, (n_wo - 2) * per_item, lambda c: stage_d(0, c, hbuf))
    loop((n_wo - 1) * per_item, chunks, lambda c: stage_c(0, c, xbuf, hbuf))
    loop((n_wo - 2) * per_item, chunks, lambda c: stage_d(0, c, hbuf))
    loop(0, chunks, lambda c: finish(0, c, hbuf))
    norm(hbuf, gm_ref)

    def gate_up(j, _):
        i = gu0 + 2 * j
        gate = product(normed, arrived(i), d)
        up = product(normed, arrived(i + 1), d)
        hidden[:, columns(j * WIDTH, WIDTH)] = (gate * (1.0 / (1.0 + jnp.exp(-gate))) * up).astype(BF16)
        issue(i + SLOTS, ("gu", "wd"))
        issue(i + 1 + SLOTS, ("gu", "wd"))
        return 0

    lax.fori_loop(0, ff // WIDTH, gate_up, 0)

    def down(c, _):
        blocks = chunk // WIDTH
        for u in range(blocks):
            i = wd0 + c * blocks + u
            part = product(hidden, arrived(i, ff), ff)
            at = u * WIDTH
            pbuf[c, at // core_cols, :, at % core_cols : at % core_cols + WIDTH] = part
            issue(i + SLOTS, ("wd",))
            if u == blocks // 2 - 1:

                @pl.when(c >= 1)
                def _():
                    stage_b(1, c - 1)

                @pl.when(c >= 2)
                def _():
                    stage_d(1, c - 2, y_ref)

        stage_a(1, c)

        @pl.when(c >= 1)
        def _():
            stage_c(1, c - 1, hbuf, y_ref)

        return 0

    lax.fori_loop(0, chunks, down, 0)
    last = chunks - 1
    stage_b(1, last)
    stage_d(1, last - 1, y_ref)
    stage_c(1, last, hbuf, y_ref)
    stage_d(1, last, y_ref)
    loop(0, chunks, lambda c: finish(1, c, y_ref))


def solution(mesh):
    n = mesh.shape["tp"]

    def step(x, k_cache, v_cache, gain_a, wq, wo, gain_m, w_gate, w_up, w_down):
        (rows, d), cache, qcols, ff = x.shape, k_cache.shape[1], wq.shape[1], w_gate.shape[1]
        half = HEAD // 2
        angle = (cache - 1) * float(THETA) ** (-np.arange(half) / half)
        cos, sin = np.cos(angle), np.sin(angle)
        rot = jnp.asarray(np.stack([np.concatenate([cos, cos]), np.concatenate([-sin, sin])]), F32)
        chips = n // CORES
        chunk = n * LANES
        chunks = d // chunk
        core_cols = chips * LANES
        any_, vmem = pl.BlockSpec(memory_space=pl.ANY), pl.BlockSpec(memory_space=pltpu.VMEM)
        dma = pltpu.SemaphoreType.DMA
        flops = 2 * rows * (2 * d * qcols + 3 * d * ff + 2 * cache * qcols)
        return pl.pallas_call(
            functools.partial(layer, n, (rows, d, cache, qcols, ff)),
            out_shape=jax.ShapeDtypeStruct((rows, d), BF16),
            in_specs=[any_, any_, any_, vmem, vmem, vmem] + [any_] * 5,
            out_specs=vmem,
            scratch_shapes=[
                pltpu.VMEM((SLOTS, d, WIDTH), BF16),
                pltpu.VMEM((rows, d), BF16),
                pltpu.VMEM((rows, d), BF16),
                pltpu.VMEM((rows, d), BF16),
                pltpu.VMEM((d // LANES, LANES), F32),
                pltpu.VMEM((rows * (qcols // HEAD), HEAD), F32),
                pltpu.VMEM((rows * (qcols // HEAD), HEAD), F32),
                pltpu.VMEM((rows, qcols), BF16),
                pltpu.VMEM((rows, ff), BF16),
                pltpu.VMEM((chunks, CORES, rows, core_cols), F32),
                pltpu.VMEM((chunks, rows, core_cols), BF16),
                pltpu.VMEM((chunks, rows, core_cols), BF16),
                pltpu.VMEM((chunks, chips, rows, LANES), BF16),
                pltpu.VMEM((chunks, chips - 1, rows, LANES), BF16),
                dma((SLOTS,)),
                dma(()),
                dma((2, chunks)),
                dma((2, chunks)),
                dma((2, chunks, chips - 1)),
                dma((2, chunks, chips - 1)),
                dma((2, chunks, chips - 1)),
                dma((2, chunks, chips - 1)),
                dma((2, chunks)),
                dma((2, chunks)),
            ],
            compiler_params=pltpu.CompilerParams(
                collective_id=0, has_side_effects=True, vmem_limit_bytes=67_043_328
            ),
            cost_estimate=pl.CostEstimate(
                flops=flops, transcendentals=0, bytes_accessed=2 * (2 * d * qcols + 3 * d * ff + 2 * rows * cache * HEAD)
            ),
        )(
            x,
            k_cache.reshape(rows, cache, HEAD),
            v_cache.reshape(rows, cache, HEAD),
            gain_a.reshape(d // LANES, LANES),
            gain_m.reshape(d // LANES, LANES),
            rot,
            wq,
            wo,
            w_gate,
            w_up,
            w_down,
        )

    states, cache, columns, rows_of = P("dp", None), P("dp", None, "tp", None), P(None, "tp"), P("tp", None)
    return jax.shard_map(
        step,
        mesh=mesh,
        in_specs=(states, cache, cache, P(None), columns, rows_of, P(None), columns, columns, rows_of),
        out_specs=states,
        check_vma=False,
    )
```

```python
import functools

import jax
import jax.numpy as jnp
import numpy as np
from jax import lax
from jax.experimental import pallas as pl
from jax.experimental.pallas import tpu as pltpu
from jax.sharding import PartitionSpec as P

HEAD = 128
THETA = 10000
LANES = 128
WIDTH = 256
SLOTS = 12
STEP = 256
CORES = 2
F32, BF16 = jnp.float32, jnp.bfloat16
MESH = pl.DeviceIdType.MESH


def layer(n, dims, x_hbm, k_hbm, v_hbm, ga_ref, gm_ref, rot_ref, wq_hbm, wo_hbm, wg_hbm, wu_hbm, wd_hbm, y_ref,
          ring, xbuf, normed, hbuf, gain, q, seen, seen_bf, hidden, pbuf, sbuf, dbuf, tbuf, rbuf,
          ring_sem, x_sem, s_a, r_a, s_b, r_b, s_c, r_c, s_d, r_d):
    rows, d, cache, qcols, ff = dims
    heads = qcols // HEAD
    half_cache = cache // 2
    group = d // half_cache
    chips = n // CORES
    chunk = CORES * chips * LANES
    chunks = d // chunk
    core_cols = chips * LANES
    wo_cols = d // qcols * WIDTH
    per_item = wo_cols // chunk

    n_q, n_kv, n_wo, n_gu, n_wd = qcols // WIDTH, 2 * rows // group, d // wo_cols, 2 * ff // WIDTH, d // WIDTH
    kv0 = n_q
    wo0 = kv0 + n_kv
    gu0 = wo0 + n_wo
    wd0 = gu0 + n_gu
    end = wd0 + n_wd

    me = lax.axis_index("tp")
    chip, core = me // CORES, me % CORES
    partner = chip * CORES + (1 - core)

    def peer(distance):
        return lax.rem(chip + distance, chips) * CORES + core

    def columns(start, size):
        return pl.ds(pl.multiple_of(start, size), size)

    def slot(i):
        return i % SLOTS if isinstance(i, int) else lax.rem(i, SLOTS)

    def issue(i, phases):
        s = slot(i)
        sem = ring_sem.at[s]

        def cols_of(w, block, height):
            pltpu.make_async_copy(w.at[:, columns(block * WIDTH, WIDTH)], ring.at[s, pl.ds(0, height)], sem).start()

        def caches(src, g):
            for t in range(group):
                for h in range(2):
                    pltpu.make_async_copy(
                        src.at[g * group + t, pl.ds(h * half_cache, half_cache)],
                        ring.at[s, pl.ds(t * half_cache, half_cache), pl.ds(h * HEAD, HEAD)],
                        sem,
                    ).start()

        def wo_blocks(w):
            for m in range(wo_cols // WIDTH):
                pltpu.make_async_copy(
                    wo_hbm.at[:, columns(w * wo_cols + m * WIDTH, WIDTH)], ring.at[s, pl.ds(m * qcols, qcols)], sem
                ).start()

        def when(low, high, body):
            if isinstance(i, int):
                if low <= i < high:
                    body()
            else:
                pl.when((i >= low) & (i < high))(body)

        def either(first, second, j):
            if isinstance(j, int):
                (second if j % 2 else first)(j // 2)
            else:
                pl.when(j % 2 == 0)(lambda: first(j // 2))
                pl.when(j % 2 == 1)(lambda: second(j // 2))

        if "q" in phases:
            when(0, kv0, lambda: cols_of(wq_hbm, i, d))
        if "kv" in phases:
            when(kv0, wo0, lambda: either(lambda g: caches(k_hbm, g), lambda g: caches(v_hbm, g), i - kv0))
        if "wo" in phases:
            when(wo0, gu0, lambda: wo_blocks(i - wo0))
        if "gu" in phases:
            when(gu0, wd0, lambda: either(lambda j: cols_of(wg_hbm, j, d), lambda j: cols_of(wu_hbm, j, d), i - gu0))
        if "wd" in phases:
            when(wd0, end, lambda: cols_of(wd_hbm, i - wd0, ff))

    def arrived(i, height=d):
        s = slot(i)
        src = wd_hbm if height == ff else wg_hbm
        pltpu.make_async_copy(src.at[:, pl.ds(0, WIDTH)], ring.at[s, pl.ds(0, height)], ring_sem.at[s]).wait()
        return s

    def products(a_ref, depth, first, second, step=STEP):
        totals = [None, None]
        for k in range(0, depth, step):
            size = min(step, depth - k)
            a = a_ref[:, k : k + size]
            for j, (s, start) in enumerate((first, second)):
                part = jnp.dot(a, ring[s, start + k : start + k + size], preferred_element_type=F32)
                totals[j] = part if totals[j] is None else totals[j] + part
        return totals

    barrier = pltpu.get_barrier_semaphore()
    for device in [partner] + [peer(dist) for dist in range(1, chips)]:
        pl.semaphore_signal(barrier, inc=1, device_id={"tp": device}, device_id_type=MESH)
    x_copy = pltpu.make_async_copy(x_hbm, xbuf, x_sem)
    x_copy.start()
    for i in range(SLOTS):
        issue(i, ("q", "kv"))

    def norm(src_ref, gain_ref):
        gain[...] = gain_ref[...].astype(F32)
        block = 2 * LANES

        def square(r, acc):
            v = src_ref[:, columns(r * block, block)].astype(F32)
            v = v * v
            return acc + (v[:, :LANES] + v[:, LANES:])

        acc = lax.fori_loop(0, d // block, square, jnp.zeros((rows, LANES), F32), unroll=4)
        scale = lax.rsqrt(jnp.sum(acc, -1, keepdims=True) * (1.0 / d) + 1e-6)
        scale = jnp.broadcast_to(scale, (rows, LANES))

        def apply(r, _):
            at = columns(r * LANES, LANES)
            normed[:, at] = (src_ref[:, at].astype(F32) * scale * gain[pl.ds(r, 1), :]).astype(BF16)
            return 0

        lax.fori_loop(0, d // LANES, apply, 0, unroll=4)

    x_copy.wait()
    norm(xbuf, ga_ref)

    def queries(p, _):
        i = 2 * p
        both = products(normed, d, (arrived(i), 0), (arrived(i + 1), 0))
        cos, sin = rot_ref[0:1, :], rot_ref[1:2, :]
        for b, t in enumerate(both):
            t = t.astype(BF16).astype(F32)
            for j in range(WIDTH // HEAD):
                one = t[:, j * HEAD : (j + 1) * HEAD]
                turned = one * cos + pltpu.roll(one, HEAD // 2, 1) * sin
                q[pl.ds((i + b) * (WIDTH // HEAD) + j, rows, stride=heads), :] = turned.astype(BF16).astype(F32)
            issue(i + b + SLOTS, ("kv",))
        return 0

    lax.fori_loop(0, n_q // 2, queries, 0)

    def attend(g, _):
        i = kv0 + 2 * g
        sk = arrived(i)
        sv = arrived(i + 1)
        weights = []
        for t in range(group):
            qb = q[pl.ds(pl.multiple_of((g * group + t) * heads, heads), heads), :]
            zero = jnp.zeros_like(qb)
            both = jnp.concatenate([jnp.concatenate([qb, zero], 1), jnp.concatenate([zero, qb], 1)], 0).astype(BF16)
            keys = ring[sk, t * half_cache : (t + 1) * half_cache]
            scores = lax.dot_general(both, keys, (((1,), (1,)), ((), ())), preferred_element_type=F32) * HEAD**-0.5
            top = jnp.max(scores, -1, keepdims=True)
            top = jnp.maximum(top[:heads], top[heads:])
            e = jnp.exp(scores - jnp.concatenate([top, top], 0))
            total = jnp.sum(e, -1, keepdims=True)
            total = 1.0 / (total[:heads] + total[heads:])
            weights.append((e * jnp.concatenate([total, total], 0)).astype(BF16))
        for t in range(group):
            values = ring[sv, t * half_cache : (t + 1) * half_cache]
            out = jnp.dot(weights[t], values, preferred_element_type=F32)
            seen[pl.ds(g * group + t, heads, stride=rows), :] = out[:heads, :HEAD] + out[heads:, HEAD:]
        issue(i + SLOTS, ("kv", "wo", "gu"))
        issue(i + 1 + SLOTS, ("kv", "wo", "gu"))
        return 0

    lax.fori_loop(0, rows // group, attend, 0)
    for h in range(heads):
        seen_bf[:, h * HEAD : (h + 1) * HEAD] = seen[h * rows : (h + 1) * rows, :].astype(BF16)

    def half_to_partner(ph, c):
        return pltpu.make_async_remote_copy(
            src_ref=sbuf.at[c], dst_ref=dbuf.at[c], send_sem=s_a.at[ph, c], recv_sem=r_a.at[ph, c],
            device_id={"tp": partner}, device_id_type=MESH)

    def term_to(ph, c, dist):
        return pltpu.make_async_remote_copy(
            src_ref=tbuf.at[c, lax.rem(chip + dist, chips)], dst_ref=rbuf.at[c, dist - 1],
            send_sem=s_b.at[ph, c, dist - 1], recv_sem=r_b.at[ph, c, dist - 1],
            device_id={"tp": peer(dist)}, device_id_type=MESH)

    def own_columns(c):
        return columns(c * chunk + core * core_cols + chip * LANES, LANES)

    def result_to(dst, ph, c, dist):
        return pltpu.make_async_remote_copy(
            src_ref=dst.at[:, own_columns(c)], dst_ref=dst.at[:, own_columns(c)],
            send_sem=s_c.at[ph, c, dist - 1], recv_sem=r_c.at[ph, c, dist - 1],
            device_id={"tp": peer(dist)}, device_id_type=MESH)

    def results_to_partner(dst, ph, c):
        at = columns(c * chunk + core * core_cols, core_cols)
        return pltpu.make_async_remote_copy(
            src_ref=dst.at[:, at], dst_ref=dst.at[:, at], send_sem=s_d.at[ph, c], recv_sem=r_d.at[ph, c],
            device_id={"tp": partner}, device_id_type=MESH)

    def stage_a(ph, c):
        sbuf[c] = pbuf[c, 1 - core].astype(BF16)
        half_to_partner(ph, c).start()

    def stage_b(ph, c):
        half_to_partner(ph, c).wait_recv()
        both = pbuf[c, core] + dbuf[c].astype(F32)
        pbuf[c, core] = both
        for p in range(chips):
            tbuf[c, p] = both[:, p * LANES : (p + 1) * LANES].astype(BF16)
        for dist in range(1, chips):
            term_to(ph, c, dist).start()

    def stage_c(ph, c, res, dst):
        for dist in range(1, chips):
            term_to(ph, c, dist).wait_recv()
        total = pbuf[c, core, :, columns(chip * LANES, LANES)]
        for dist in range(1, chips):
            total = total + rbuf[c, dist - 1].astype(F32)
        at = own_columns(c)
        dst[:, at] = (res[:, at].astype(F32) + total).astype(BF16)
        for dist in range(1, chips):
            result_to(dst, ph, c, dist).start()

    def stage_d(ph, c, dst):
        for dist in range(1, chips):
            result_to(dst, ph, c, dist).wait_recv()
        results_to_partner(dst, ph, c).start()

    def finish(ph, c, dst):
        results_to_partner(dst, ph, c).wait()
        half_to_partner(ph, c).wait_send()
        for dist in range(1, chips):
            term_to(ph, c, dist).wait_send()
            result_to(dst, ph, c, dist).wait_send()

    def loop(low, high, body):
        lax.fori_loop(low, high, lambda c, _: (body(c), 0)[1], 0)

    pl.semaphore_wait(barrier, chips)

    def project(w, _):
        i = wo0 + w
        s = arrived(i)
        for m in range(0, wo_cols // WIDTH, 2):
            c = w * per_item + m * WIDTH // chunk
            for b, part in enumerate(products(seen_bf, qcols, (s, m * qcols), (s, (m + 1) * qcols))):
                at = (m + b) * WIDTH % chunk
                pbuf[c, at // core_cols, :, at % core_cols : at % core_cols + WIDTH] = part
            if (m + 2) * WIDTH % chunk == 0:
                stage_a(0, c)
        issue(i + SLOTS, ("gu",))

        @pl.when(w >= 1)
        def _():
            for j in range(per_item):
                stage_b(0, (w - 1) * per_item + j)

        @pl.when(w >= 2)
        def _():
            for j in range(per_item):
                stage_c(0, (w - 2) * per_item + j, xbuf, hbuf)

        return 0

    lax.fori_loop(0, n_wo, project, 0)
    loop((n_wo - 1) * per_item, chunks, lambda c: stage_b(0, c))
    loop((n_wo - 2) * per_item, (n_wo - 1) * per_item, lambda c: stage_c(0, c, xbuf, hbuf))
    loop(0, (n_wo - 2) * per_item, lambda c: stage_d(0, c, hbuf))
    loop((n_wo - 1) * per_item, chunks, lambda c: stage_c(0, c, xbuf, hbuf))
    loop((n_wo - 2) * per_item, chunks, lambda c: stage_d(0, c, hbuf))
    loop(0, chunks, lambda c: finish(0, c, hbuf))
    norm(hbuf, gm_ref)

    def gate_up(j, _):
        i = gu0 + 2 * j
        gate, up = products(normed, d, (arrived(i), 0), (arrived(i + 1), 0))
        hidden[:, columns(j * WIDTH, WIDTH)] = (gate * (1.0 / (1.0 + jnp.exp(-gate))) * up).astype(BF16)
        issue(i + SLOTS, ("gu", "wd"))
        issue(i + 1 + SLOTS, ("gu", "wd"))
        return 0

    lax.fori_loop(0, ff // WIDTH, gate_up, 0)

    def down(c, _):
        blocks = chunk // WIDTH
        for u in range(0, blocks, 2):
            i = wd0 + c * blocks + u
            for b, part in enumerate(products(hidden, ff, (arrived(i, ff), 0), (arrived(i + 1, ff), 0))):
                at = (u + b) * WIDTH
                pbuf[c, at // core_cols, :, at % core_cols : at % core_cols + WIDTH] = part
            issue(i + SLOTS, ("wd",))
            issue(i + 1 + SLOTS, ("wd",))
            if u == 0:

                @pl.when(c >= 1)
                def _():
                    stage_b(1, c - 1)

                @pl.when(c >= 2)
                def _():
                    stage_c(1, c - 2, hbuf, y_ref)

                @pl.when(c >= 3)
                def _():
                    stage_d(1, c - 3, y_ref)

        stage_a(1, c)
        return 0

    lax.fori_loop(0, chunks, down, 0)
    last = chunks - 1
    stage_c(1, last - 1, hbuf, y_ref)
    stage_b(1, last)
    stage_d(1, last - 2, y_ref)
    stage_d(1, last - 1, y_ref)
    stage_c(1, last, hbuf, y_ref)
    stage_d(1, last, y_ref)
    loop(0, chunks, lambda c: finish(1, c, y_ref))


def solution(mesh):
    n = mesh.shape["tp"]

    def step(x, k_cache, v_cache, gain_a, wq, wo, gain_m, w_gate, w_up, w_down):
        (rows, d), cache, qcols, ff = x.shape, k_cache.shape[1], wq.shape[1], w_gate.shape[1]
        half = HEAD // 2
        angle = (cache - 1) * float(THETA) ** (-np.arange(half) / half)
        cos, sin = np.cos(angle), np.sin(angle)
        rot = jnp.asarray(np.stack([np.concatenate([cos, cos]), np.concatenate([-sin, sin])]), F32)
        chips = n // CORES
        chunk = n * LANES
        chunks = d // chunk
        core_cols = chips * LANES
        any_, vmem = pl.BlockSpec(memory_space=pl.ANY), pl.BlockSpec(memory_space=pltpu.VMEM)
        dma = pltpu.SemaphoreType.DMA
        flops = 2 * rows * (2 * d * qcols + 3 * d * ff + 2 * cache * qcols)
        return pl.pallas_call(
            functools.partial(layer, n, (rows, d, cache, qcols, ff)),
            out_shape=jax.ShapeDtypeStruct((rows, d), BF16),
            in_specs=[any_, any_, any_, vmem, vmem, vmem] + [any_] * 5,
            out_specs=vmem,
            scratch_shapes=[
                pltpu.VMEM((SLOTS, d, WIDTH), BF16),
                pltpu.VMEM((rows, d), BF16),
                pltpu.VMEM((rows, d), BF16),
                pltpu.VMEM((rows, d), BF16),
                pltpu.VMEM((d // LANES, LANES), F32),
                pltpu.VMEM((rows * (qcols // HEAD), HEAD), F32),
                pltpu.VMEM((rows * (qcols // HEAD), HEAD), F32),
                pltpu.VMEM((rows, qcols), BF16),
                pltpu.VMEM((rows, ff), BF16),
                pltpu.VMEM((chunks, CORES, rows, core_cols), F32),
                pltpu.VMEM((chunks, rows, core_cols), BF16),
                pltpu.VMEM((chunks, rows, core_cols), BF16),
                pltpu.VMEM((chunks, chips, rows, LANES), BF16),
                pltpu.VMEM((chunks, chips - 1, rows, LANES), BF16),
                dma((SLOTS,)),
                dma(()),
                dma((2, chunks)),
                dma((2, chunks)),
                dma((2, chunks, chips - 1)),
                dma((2, chunks, chips - 1)),
                dma((2, chunks, chips - 1)),
                dma((2, chunks, chips - 1)),
                dma((2, chunks)),
                dma((2, chunks)),
            ],
            compiler_params=pltpu.CompilerParams(
                collective_id=0, has_side_effects=True, vmem_limit_bytes=67_043_328
            ),
            cost_estimate=pl.CostEstimate(
                flops=flops, transcendentals=0, bytes_accessed=2 * (2 * d * qcols + 3 * d * ff + 2 * rows * cache * HEAD)
            ),
        )(
            x,
            k_cache.reshape(rows, cache, HEAD),
            v_cache.reshape(rows, cache, HEAD),
            gain_a.reshape(d // LANES, LANES),
            gain_m.reshape(d // LANES, LANES),
            rot,
            wq,
            wo,
            w_gate,
            w_up,
            w_down,
        )

    states, cache, columns, rows_of = P("dp", None), P("dp", None, "tp", None), P(None, "tp"), P("tp", None)
    return jax.shard_map(
        step,
        mesh=mesh,
        in_specs=(states, cache, cache, P(None), columns, rows_of, P(None), columns, columns, rows_of),
        out_specs=states,
        check_vma=False,
    )
```

```python
import functools

import jax
import jax.numpy as jnp
import numpy as np
from jax import lax
from jax.experimental import pallas as pl
from jax.experimental.pallas import tpu as pltpu
from jax.sharding import PartitionSpec as P

HEAD = 128
THETA = 10000
LANES = 128
WIDTH = 256
SLOTS = 12
STEP = 256
CORES = 2
F32, BF16 = jnp.float32, jnp.bfloat16
MESH = pl.DeviceIdType.MESH


def layer(n, dims, x_hbm, k_hbm, v_hbm, ga_ref, gm_ref, rot_ref, wq_hbm, wo_hbm, wg_hbm, wu_hbm, wd_hbm, y_ref,
          ring, xbuf, normed, hbuf, gain, q, seen, seen_bf, hidden, pbuf, sbuf, dbuf, tbuf, rbuf,
          ring_sem, x_sem, s_a, r_a, s_b, r_b, s_c, r_c, s_d, r_d):
    rows, d, cache, qcols, ff = dims
    heads = qcols // HEAD
    half_cache = cache // 2
    group = d // half_cache
    chips = n // CORES
    chunk = CORES * chips * LANES
    chunks = d // chunk
    core_cols = chips * LANES
    wo_cols = d // qcols * WIDTH
    per_item = wo_cols // chunk

    n_q, n_kv, n_wo, n_gu, n_wd = qcols // WIDTH, 2 * rows // group, d // wo_cols, 2 * ff // WIDTH, d // WIDTH
    kv0 = n_q
    wo0 = kv0 + n_kv
    gu0 = wo0 + n_wo
    wd0 = gu0 + n_gu
    end = wd0 + n_wd

    me = lax.axis_index("tp")
    chip, core = me // CORES, me % CORES
    partner = chip * CORES + (1 - core)

    def peer(distance):
        return lax.rem(chip + distance, chips) * CORES + core

    def columns(start, size):
        return pl.ds(pl.multiple_of(start, size), size)

    def slot(i):
        return i % SLOTS if isinstance(i, int) else lax.rem(i, SLOTS)

    def issue(i, phases):
        s = slot(i)
        sem = ring_sem.at[s]

        def cols_of(w, block, height):
            pltpu.make_async_copy(w.at[:, columns(block * WIDTH, WIDTH)], ring.at[s, pl.ds(0, height)], sem).start()

        def caches(src, g):
            for t in range(group):
                for h in range(2):
                    pltpu.make_async_copy(
                        src.at[g * group + t, pl.ds(h * half_cache, half_cache)],
                        ring.at[s, pl.ds(t * half_cache, half_cache), pl.ds(h * HEAD, HEAD)],
                        sem,
                    ).start()

        def wo_blocks(w):
            for m in range(wo_cols // WIDTH):
                pltpu.make_async_copy(
                    wo_hbm.at[:, columns(w * wo_cols + m * WIDTH, WIDTH)], ring.at[s, pl.ds(m * qcols, qcols)], sem
                ).start()

        def when(low, high, body):
            if isinstance(i, int):
                if low <= i < high:
                    body()
            else:
                pl.when((i >= low) & (i < high))(body)

        def either(first, second, j):
            if isinstance(j, int):
                (second if j % 2 else first)(j // 2)
            else:
                pl.when(j % 2 == 0)(lambda: first(j // 2))
                pl.when(j % 2 == 1)(lambda: second(j // 2))

        if "q" in phases:
            when(0, kv0, lambda: cols_of(wq_hbm, i, d))
        if "kv" in phases:
            when(kv0, wo0, lambda: either(lambda g: caches(k_hbm, g), lambda g: caches(v_hbm, g), i - kv0))
        if "wo" in phases:
            when(wo0, gu0, lambda: wo_blocks(i - wo0))
        if "gu" in phases:
            when(gu0, wd0, lambda: either(lambda j: cols_of(wg_hbm, j, d), lambda j: cols_of(wu_hbm, j, d), i - gu0))
        if "wd" in phases:
            when(wd0, end, lambda: cols_of(wd_hbm, i - wd0, ff))

    def arrived(i, height=d):
        s = slot(i)
        src = wd_hbm if height == ff else wg_hbm
        pltpu.make_async_copy(src.at[:, pl.ds(0, WIDTH)], ring.at[s, pl.ds(0, height)], ring_sem.at[s]).wait()
        return s

    def products(a_ref, depth, first, second, step=STEP):
        totals = [None, None]
        for k in range(0, depth, step):
            size = min(step, depth - k)
            a = a_ref[:, k : k + size]
            for j, (s, start) in enumerate((first, second)):
                part = jnp.dot(a, ring[s, start + k : start + k + size], preferred_element_type=F32)
                totals[j] = part if totals[j] is None else totals[j] + part
        return totals

    barrier = pltpu.get_barrier_semaphore()
    for device in [partner] + [peer(dist) for dist in range(1, chips)]:
        pl.semaphore_signal(barrier, inc=1, device_id={"tp": device}, device_id_type=MESH)
    x_copy = pltpu.make_async_copy(x_hbm, xbuf, x_sem)
    x_copy.start()
    for i in range(SLOTS):
        issue(i, ("q", "kv"))

    def norm(src_ref, gain_ref):
        gain[...] = gain_ref[...].astype(F32)
        block = 2 * LANES

        def square(r, acc):
            v = src_ref[:, columns(r * block, block)].astype(F32)
            v = v * v
            return acc + (v[:, :LANES] + v[:, LANES:])

        acc = lax.fori_loop(0, d // block, square, jnp.zeros((rows, LANES), F32), unroll=4)
        scale = lax.rsqrt(jnp.sum(acc, -1, keepdims=True) * (1.0 / d) + 1e-6)
        scale = jnp.broadcast_to(scale, (rows, LANES))

        def apply(r, _):
            at = columns(r * LANES, LANES)
            normed[:, at] = (src_ref[:, at].astype(F32) * scale * gain[pl.ds(r, 1), :]).astype(BF16)
            return 0

        lax.fori_loop(0, d // LANES, apply, 0, unroll=4)

    x_copy.wait()
    norm(xbuf, ga_ref)

    def queries(p, _):
        i = 2 * p
        both = products(normed, d, (arrived(i), 0), (arrived(i + 1), 0))
        cos, sin = rot_ref[0:1, :], rot_ref[1:2, :]
        for b, t in enumerate(both):
            t = t.astype(BF16).astype(F32)
            for j in range(WIDTH // HEAD):
                one = t[:, j * HEAD : (j + 1) * HEAD]
                turned = one * cos + pltpu.roll(one, HEAD // 2, 1) * sin
                q[pl.ds((i + b) * (WIDTH // HEAD) + j, rows, stride=heads), :] = turned.astype(BF16).astype(F32)
            issue(i + b + SLOTS, ("kv",))
        return 0

    lax.fori_loop(0, n_q // 2, queries, 0)

    def attend(g, _):
        i = kv0 + 2 * g
        sk = arrived(i)
        sv = arrived(i + 1)
        weights = []
        for t in range(group):
            qb = q[pl.ds(pl.multiple_of((g * group + t) * heads, heads), heads), :]
            zero = jnp.zeros_like(qb)
            both = jnp.concatenate([jnp.concatenate([qb, zero], 1), jnp.concatenate([zero, qb], 1)], 0).astype(BF16)
            keys = ring[sk, t * half_cache : (t + 1) * half_cache]
            scores = lax.dot_general(both, keys, (((1,), (1,)), ((), ())), preferred_element_type=F32) * HEAD**-0.5
            top = jnp.max(scores, -1, keepdims=True)
            top = jnp.maximum(top[:heads], top[heads:])
            e = jnp.exp(scores - jnp.concatenate([top, top], 0))
            total = jnp.sum(e, -1, keepdims=True)
            total = 1.0 / (total[:heads] + total[heads:])
            weights.append((e * jnp.concatenate([total, total], 0)).astype(BF16))
        for t in range(group):
            values = ring[sv, t * half_cache : (t + 1) * half_cache]
            out = jnp.dot(weights[t], values, preferred_element_type=F32)
            seen[pl.ds(g * group + t, heads, stride=rows), :] = out[:heads, :HEAD] + out[heads:, HEAD:]
        issue(i + SLOTS, ("kv", "wo", "gu"))
        issue(i + 1 + SLOTS, ("kv", "wo", "gu"))
        return 0

    lax.fori_loop(0, rows // group, attend, 0)
    for h in range(heads):
        seen_bf[:, h * HEAD : (h + 1) * HEAD] = seen[h * rows : (h + 1) * rows, :].astype(BF16)

    def half_to_partner(ph, c):
        return pltpu.make_async_remote_copy(
            src_ref=sbuf.at[c], dst_ref=dbuf.at[c], send_sem=s_a.at[ph, c], recv_sem=r_a.at[ph, c],
            device_id={"tp": partner}, device_id_type=MESH)

    def term_to(ph, c, dist):
        return pltpu.make_async_remote_copy(
            src_ref=tbuf.at[c, lax.rem(chip + dist, chips)], dst_ref=rbuf.at[c, dist - 1],
            send_sem=s_b.at[ph, c, dist - 1], recv_sem=r_b.at[ph, c, dist - 1],
            device_id={"tp": peer(dist)}, device_id_type=MESH)

    def own_columns(c):
        return columns(c * chunk + core * core_cols + chip * LANES, LANES)

    def result_to(dst, ph, c, dist):
        return pltpu.make_async_remote_copy(
            src_ref=dst.at[:, own_columns(c)], dst_ref=dst.at[:, own_columns(c)],
            send_sem=s_c.at[ph, c, dist - 1], recv_sem=r_c.at[ph, c, dist - 1],
            device_id={"tp": peer(dist)}, device_id_type=MESH)

    def results_to_partner(dst, ph, c):
        at = columns(c * chunk + core * core_cols, core_cols)
        return pltpu.make_async_remote_copy(
            src_ref=dst.at[:, at], dst_ref=dst.at[:, at], send_sem=s_d.at[ph, c], recv_sem=r_d.at[ph, c],
            device_id={"tp": partner}, device_id_type=MESH)

    def stage_a(ph, c):
        sbuf[c] = pbuf[c, 1 - core].astype(BF16)
        half_to_partner(ph, c).start()

    def stage_b(ph, c):
        half_to_partner(ph, c).wait_recv()
        both = pbuf[c, core] + dbuf[c].astype(F32)
        pbuf[c, core] = both
        for p in range(chips):
            tbuf[c, p] = both[:, p * LANES : (p + 1) * LANES].astype(BF16)
        for dist in range(1, chips):
            term_to(ph, c, dist).start()

    def stage_c(ph, c, res, dst):
        for dist in range(1, chips):
            term_to(ph, c, dist).wait_recv()
        total = pbuf[c, core, :, columns(chip * LANES, LANES)]
        for dist in range(1, chips):
            total = total + rbuf[c, dist - 1].astype(F32)
        at = own_columns(c)
        dst[:, at] = (res[:, at].astype(F32) + total).astype(BF16)
        for dist in range(1, chips):
            result_to(dst, ph, c, dist).start()

    def stage_d(ph, c, dst):
        for dist in range(1, chips):
            result_to(dst, ph, c, dist).wait_recv()
        results_to_partner(dst, ph, c).start()

    def finish(ph, c, dst):
        results_to_partner(dst, ph, c).wait()
        half_to_partner(ph, c).wait_send()
        for dist in range(1, chips):
            term_to(ph, c, dist).wait_send()
            result_to(dst, ph, c, dist).wait_send()

    def loop(low, high, body):
        lax.fori_loop(low, high, lambda c, _: (body(c), 0)[1], 0)

    pl.semaphore_wait(barrier, chips)

    def project(w, _):
        i = wo0 + w
        s = arrived(i)
        for m in range(0, wo_cols // WIDTH, 2):
            c = w * per_item + m * WIDTH // chunk
            for b, part in enumerate(products(seen_bf, qcols, (s, m * qcols), (s, (m + 1) * qcols))):
                at = (m + b) * WIDTH % chunk
                pbuf[c, at // core_cols, :, at % core_cols : at % core_cols + WIDTH] = part
            if (m + 2) * WIDTH % chunk == 0:
                stage_a(0, c)
        issue(i + SLOTS, ("gu",))

        @pl.when(w >= 1)
        def _():
            for j in range(per_item):
                stage_b(0, (w - 1) * per_item + j)

        return 0

    lax.fori_loop(0, n_wo, project, 0)
    loop((n_wo - 1) * per_item, chunks, lambda c: stage_b(0, c))
    late = (n_wo - 1) * per_item
    loop(0, late, lambda c: stage_c(0, c, xbuf, hbuf))
    loop(0, late - per_item, lambda c: stage_d(0, c, hbuf))
    loop(late, chunks, lambda c: stage_c(0, c, xbuf, hbuf))
    loop(late - per_item, chunks, lambda c: stage_d(0, c, hbuf))
    loop(0, chunks, lambda c: finish(0, c, hbuf))
    norm(hbuf, gm_ref)

    def gate_up(j, _):
        i = gu0 + 2 * j
        gate, up = products(normed, d, (arrived(i), 0), (arrived(i + 1), 0))
        hidden[:, columns(j * WIDTH, WIDTH)] = (gate * (1.0 / (1.0 + jnp.exp(-gate))) * up).astype(BF16)
        issue(i + SLOTS, ("gu", "wd"))
        issue(i + 1 + SLOTS, ("gu", "wd"))
        return 0

    lax.fori_loop(0, ff // WIDTH, gate_up, 0)

    def down(c, _):
        blocks = chunk // WIDTH
        for u in range(0, blocks, 2):
            i = wd0 + c * blocks + u
            for b, part in enumerate(products(hidden, ff, (arrived(i, ff), 0), (arrived(i + 1, ff), 0))):
                at = (u + b) * WIDTH
                pbuf[c, at // core_cols, :, at % core_cols : at % core_cols + WIDTH] = part
            issue(i + SLOTS, ("wd",))
            issue(i + 1 + SLOTS, ("wd",))

        stage_a(1, c)

        @pl.when(c >= 1)
        def _():
            stage_b(1, c - 1)

        @pl.when(c >= 2)
        def _():
            stage_c(1, c - 2, hbuf, y_ref)

        @pl.when(c >= 3)
        def _():
            stage_d(1, c - 3, y_ref)

        return 0

    lax.fori_loop(0, chunks, down, 0)
    last = chunks - 1
    stage_b(1, last)
    stage_c(1, last - 1, hbuf, y_ref)
    stage_d(1, last - 2, y_ref)
    stage_c(1, last, hbuf, y_ref)
    stage_d(1, last - 1, y_ref)
    stage_d(1, last, y_ref)
    loop(0, chunks, lambda c: finish(1, c, y_ref))


def solution(mesh):
    n = mesh.shape["tp"]

    def step(x, k_cache, v_cache, gain_a, wq, wo, gain_m, w_gate, w_up, w_down):
        (rows, d), cache, qcols, ff = x.shape, k_cache.shape[1], wq.shape[1], w_gate.shape[1]
        half = HEAD // 2
        angle = (cache - 1) * float(THETA) ** (-np.arange(half) / half)
        cos, sin = np.cos(angle), np.sin(angle)
        rot = jnp.asarray(np.stack([np.concatenate([cos, cos]), np.concatenate([-sin, sin])]), F32)
        chips = n // CORES
        chunk = n * LANES
        chunks = d // chunk
        core_cols = chips * LANES
        any_, vmem = pl.BlockSpec(memory_space=pl.ANY), pl.BlockSpec(memory_space=pltpu.VMEM)
        dma = pltpu.SemaphoreType.DMA
        flops = 2 * rows * (2 * d * qcols + 3 * d * ff + 2 * cache * qcols)
        return pl.pallas_call(
            functools.partial(layer, n, (rows, d, cache, qcols, ff)),
            out_shape=jax.ShapeDtypeStruct((rows, d), BF16),
            in_specs=[any_, any_, any_, vmem, vmem, vmem] + [any_] * 5,
            out_specs=vmem,
            scratch_shapes=[
                pltpu.VMEM((SLOTS, d, WIDTH), BF16),
                pltpu.VMEM((rows, d), BF16),
                pltpu.VMEM((rows, d), BF16),
                pltpu.VMEM((rows, d), BF16),
                pltpu.VMEM((d // LANES, LANES), F32),
                pltpu.VMEM((rows * (qcols // HEAD), HEAD), F32),
                pltpu.VMEM((rows * (qcols // HEAD), HEAD), F32),
                pltpu.VMEM((rows, qcols), BF16),
                pltpu.VMEM((rows, ff), BF16),
                pltpu.VMEM((chunks, CORES, rows, core_cols), F32),
                pltpu.VMEM((chunks, rows, core_cols), BF16),
                pltpu.VMEM((chunks, rows, core_cols), BF16),
                pltpu.VMEM((chunks, chips, rows, LANES), BF16),
                pltpu.VMEM((chunks, chips - 1, rows, LANES), BF16),
                dma((SLOTS,)),
                dma(()),
                dma((2, chunks)),
                dma((2, chunks)),
                dma((2, chunks, chips - 1)),
                dma((2, chunks, chips - 1)),
                dma((2, chunks, chips - 1)),
                dma((2, chunks, chips - 1)),
                dma((2, chunks)),
                dma((2, chunks)),
            ],
            compiler_params=pltpu.CompilerParams(
                collective_id=0, has_side_effects=True, vmem_limit_bytes=67_043_328
            ),
            cost_estimate=pl.CostEstimate(
                flops=flops, transcendentals=0, bytes_accessed=2 * (2 * d * qcols + 3 * d * ff + 2 * rows * cache * HEAD)
            ),
        )(
            x,
            k_cache.reshape(rows, cache, HEAD),
            v_cache.reshape(rows, cache, HEAD),
            gain_a.reshape(d // LANES, LANES),
            gain_m.reshape(d // LANES, LANES),
            rot,
            wq,
            wo,
            w_gate,
            w_up,
            w_down,
        )

    states, cache, columns, rows_of = P("dp", None), P("dp", None, "tp", None), P(None, "tp"), P("tp", None)
    return jax.shard_map(
        step,
        mesh=mesh,
        in_specs=(states, cache, cache, P(None), columns, rows_of, P(None), columns, columns, rows_of),
        out_specs=states,
        check_vma=False,
    )
```
